32 devices in a mesh: grp: 2 (over x), tm: 16 (over z, y, core).
Axes of the slice: x: 2, y: 2, z: 4, core: 2. Of those that a mesh axis runs over, the one named last changes fastest.
Arguments:
- visibilities: float32 [2048, 2, 16, 1024], P('tm', None, 'grp'), parts along dimension 2, may hold values from -6 to 6
- redundancy: int32 [2048], P('grp'), parts along dimension 0, may hold values from 0 to 511, as said below
- mode_counts: int32 [2048], P('tm'), may hold values from 4 to 16
- filters: bfloat16 [2048, 2, 16, 16, 512], P('tm', None, None, 'grp'), parts along dimension 3, may hold values from -0.0625 to 0.0625
Outputs:
- mmodes: float32 [2048, 2, 16, 512], P('tm', None, 'grp'), parts along dimension 2
- modes: float32 [2048, 2, 32], P('tm', None, 'grp'), parts along dimension 2
The draws below stay inside these ranges and needn't reach their ends.
There are 2 independent parts, one for each index of `grp`. The reference program is written for one: setup_inputs(seed, part) draws one part's arguments, and reference() takes and returns one part's arrays. A program takes and returns all parts, laid end to end along the dimension named above; an argument that names none is the same for every part. Nothing has to cross between parts.
Inputs may be any that keep to these rules, and one draw needn't show every extreme that they name: `redundancy`: each of the 512 unique baselines is named by at least one raw baseline.
All inputs are finite; a program needn't handle non-finite values.
Results may differ from the reference program's by a relative error of at most 0.0029.
Values sent between devices are 32-bit elements; how exact they have to be, the bound alone decides.
A program may use at most 128 MiB of HBM per device.

```python
import jax
import jax.numpy as jnp
from jax import lax

TIMES = 2048
NRAW = 1024
B = 512
F = 8
K = 16


def draw_redundancy(key, part):
    base_key = jax.random.fold_in(key, 11)
    perm_key, extra_key, order_key = jax.random.split(base_key, 3)
    covering = jax.random.permutation(perm_key, B).astype(jnp.int32)
    extras = jax.random.randint(extra_key, (NRAW - B,), 0, B).astype(jnp.int32)
    combined = jnp.concatenate([covering, extras])
    shuffle = jax.random.permutation(order_key, NRAW)
    return combined[shuffle].astype(jnp.int32)


def place_ends(result, key, smallest, top_value):
    place = [jax.random.randint(jax.random.fold_in(key, axis), (), 0, length) for axis, length in enumerate(result.shape)]
    main_axis = result.shape.index(max(result.shape))
    next_to = place[:main_axis] + [(place[main_axis] + 1) % result.shape[main_axis]] + place[main_axis + 1:]
    return result.at[tuple(place)].set(smallest).at[tuple(next_to)].set(top_value)


def level_of(key, dims, shards, low, top_value):
    level = 1.0
    for position, parts in shards:
        steps = jax.random.uniform(jax.random.fold_in(jax.random.fold_in(key, 6), position), (parts,), jnp.float32, low / len(shards), top_value / len(shards))
        level = level * jnp.repeat(jnp.exp(steps), dims[position] // parts).reshape((-1,) + (1,) * (len(dims) - 1 - position))
    return level


def scatter_about(key, dims, width, bound, cuts=(), kind=jnp.bfloat16):
    factor_of = level_of(key, dims, cuts, -0.22, 0.18) if cuts else 1.0
    entries = jax.random.normal(key, dims, jnp.float32) * width * factor_of
    return jnp.minimum(jnp.maximum(entries, -bound), bound).astype(kind)


def setup_inputs(seed: int = 0, part: int = 0) -> dict:
    streams_of = jax.random.split(jax.random.key(seed), 5)
    part_splits = jax.random.split(jax.random.fold_in(streams_of[4], part), 5)
    return {
        "visibilities": scatter_about(part_splits[0], (TIMES, 2, F, NRAW), 1.0, 6.0, ((0, 16),), jnp.float32),
        "redundancy": draw_redundancy(jax.random.fold_in(jax.random.fold_in(streams_of[4], part), 71), part),
        "mode_counts": place_ends(jax.random.randint(streams_of[2], (TIMES,), K // 4, K + 1), jax.random.fold_in(streams_of[2], 1), K // 4, K).astype(jnp.int32),
        "filters": scatter_about(part_splits[3], (TIMES, 2, K, F, B), (2 * F * B) ** -0.5, 0.0625, ((0, 16),)),
    }


def project(pieces):
    filt_block, data_block = pieces
    products = jnp.einsum("mpkc,mqc->mpqk", filt_block.astype(jnp.float32), data_block, precision=lax.Precision.HIGHEST)
    real_out = products[:, 0, 0] - products[:, 1, 1]
    imag_out = products[:, 0, 1] + products[:, 1, 0]
    return jnp.stack([real_out, imag_out], axis=1)


def reference(visibilities, redundancy, mode_counts, filters):
    uniques = filters.shape[4]
    kept = filters.shape[2]
    members = (redundancy[:, None] == jnp.arange(uniques, dtype=jnp.int32)[None, :]).astype(jnp.float32)
    summed = jnp.einsum("tpfr,rb->tpfb", visibilities, members, precision=lax.Precision.HIGHEST)
    averaged = summed / jnp.sum(members, axis=0)
    spectra = jnp.fft.fft(averaged[:, 0] + 1j * averaged[:, 1], axis=0, norm="ortho")
    mmodes = jnp.stack([jnp.real(spectra), jnp.imag(spectra)], axis=1).astype(jnp.float32)
    rounded = lax.optimization_barrier(mmodes.astype(jnp.bfloat16)).astype(jnp.float32)
    blocks = TIMES // 64
    data_blocks = rounded.reshape(blocks, 64, 2, -1)
    filt_blocks = filters.reshape(blocks, 64, 2, kept, -1)
    coefs = lax.map(project, (filt_blocks, data_blocks)).reshape(TIMES, 2, kept)
    kept_mask = jnp.arange(kept, dtype=jnp.int32)[None, :] < mode_counts[:, None]
    modes = jnp.where(kept_mask[:, None, :], coefs, 0.0).astype(jnp.float32)
    return mmodes, modes
```

```python
import functools

import numpy as np
import jax
import jax.numpy as jnp
from jax import lax
from jax.experimental import pallas as pl
from jax.experimental.pallas import tpu as pltpu
from jax.sharding import PartitionSpec as P

MESH = pl.DeviceIdType.MESH
LANES = 128
BLOCKS = 4
NT = (((1,), (1,)), ((), ()))


def split_bf16(x):
    high = x.astype(jnp.bfloat16)
    return high, (x - high.astype(jnp.float32)).astype(jnp.bfloat16)


def cmul_const(z, c):
    re, im = z
    if c == 1:
        return z
    if c == -1j:
        return im, -re
    cr, ci = float(c.real), float(c.imag)
    if abs(abs(cr) - abs(ci)) < 1e-12:
        return (re - im) * cr if ci * cr > 0 else (re + im) * cr, (re + im) * cr if ci * cr > 0 else (im - re) * cr
    return re * cr - im * ci, re * ci + im * cr


def small_fft(zs):
    n = len(zs)
    if n == 1:
        return zs
    half = n // 2
    tops = [(a[0] + b[0], a[1] + b[1]) for a, b in zip(zs[:half], zs[half:])]
    lows = [(a[0] - b[0], a[1] - b[1]) for a, b in zip(zs[:half], zs[half:])]
    turned = []
    for i, z in enumerate(lows):
        if i == 0:
            c = 1
        elif 4 * i == n:
            c = -1j
        else:
            c = np.exp(-2j * np.pi * i / n)
        turned.append(cmul_const(z, c))
    even, odd = small_fft(tops), small_fft(turned)
    out = [None] * n
    out[0::2], out[1::2] = even, odd
    return out


def tables(groups, local):
    length = groups * local
    s = np.arange(local, dtype=np.int64)
    base = 2 * np.pi * (np.outer(s, s) % local) / local
    turn = 2 * np.pi * np.outer(np.arange(groups, dtype=np.int64), s) / length
    scale = length ** -0.5
    f32 = lambda a: jnp.asarray(a.astype(np.float32))
    return (
        f32(np.cos(base) * scale),
        f32(np.sin(base) * scale),
        f32(np.cos(turn).reshape(groups, 1, local)),
        f32(np.sin(turn).reshape(groups, 1, local)),
    )


def exchange_kernel(
    n, local, chans, uniq,
    vis_ref, red_ref, cb_ref, sb_ref, tc_ref, ts_ref, out_ref,
    vis_buf, wt, avg, send1, recv1, spec, mh, ml, send2,
    load_sem, s1_sem, r1_sem, s2_sem, r2_sem, own1_sem, own2_sem,
):
    me = lax.axis_index("tm")
    halves = uniq // (n // chans) // LANES
    per_chan = n // chans
    tb = local // BLOCKS
    rows = tb * 2 * chans
    keep = local // n

    def load(i):
        return pltpu.make_async_copy(
            vis_ref.at[pl.ds(i * rows, rows), :], vis_buf.at[i], load_sem.at[i]
        )

    for i in range(BLOCKS):
        load(i).start()

    barrier = pltpu.get_barrier_semaphore()

    def greet(o, carry):
        pl.semaphore_signal(
            barrier, inc=1, device_id={"tm": lax.rem(me + o, n)}, device_id_type=MESH
        )
        return carry

    lax.fori_loop(1, n, greet, 0)

    wt[...] = (
        lax.broadcasted_iota(jnp.int32, wt.shape, 0) == red_ref[...]
    ).astype(jnp.float32).astype(jnp.bfloat16)
    ones = jnp.ones((8, wt.shape[1]), jnp.bfloat16)
    counts = lax.dot_general(ones, wt[...], NT, preferred_element_type=jnp.float32)
    inverse = 1.0 / counts[0:1]

    def slot(dest, h):
        return lax.rem(dest, per_chan) * halves + h, lax.div(dest, per_chan)

    def first(o, h, i):
        dest = lax.rem(me + o, n)
        lane_tile, chan = slot(dest, h)
        if h == 0:
            span = pl.ds(i * tb, tb)
            q = i
        else:
            span = pl.ds(0, local)
            q = BLOCKS + h - 1
        return pltpu.make_async_remote_copy(
            src_ref=send1.at[lane_tile, chan, :, span, :],
            dst_ref=recv1.at[h, me, :, span, :],
            send_sem=s1_sem.at[o, q],
            recv_sem=r1_sem.at[o, q],
            device_id={"tm": dest},
            device_id_type=MESH,
        )

    def own_first(h):
        lane_tile, chan = slot(me, h)
        return pltpu.make_async_copy(
            send1.at[lane_tile, chan], recv1.at[h, me], own1_sem.at[h]
        )

    def each(f):
        def body(o, carry):
            f(o)
            return carry
        lax.fori_loop(1, n, body, 0)

    for i in range(BLOCKS):
        load(i).wait()
        high, low = split_bf16(vis_buf[i])
        summed = lax.dot_general(high, wt[...], NT, preferred_element_type=jnp.float32)
        summed += lax.dot_general(low, wt[...], NT, preferred_element_type=jnp.float32)
        mean = summed * inverse
        for lt in range(uniq // LANES):
            avg[lt] = mean[:, lt * LANES:(lt + 1) * LANES]
        for lt in range(uniq // LANES):
            for f in range(chans):
                for p in range(2):
                    send1[lt, f, p, i * tb:(i + 1) * tb, :] = avg[
                        lt, pl.ds(p * chans + f, tb, stride=2 * chans), :
                    ]
        if i == 0:
            pl.semaphore_wait(barrier, n - 1)
        each(lambda o: first(o, 0, i).start())
    for h in range(1, halves):
        each(lambda o: first(o, h, 0).start())
    for h in range(halves):
        own_first(h).start()

    def make_matrix(e, carry):
        cosine = cb_ref[...] * tc_ref[e] - sb_ref[...] * ts_ref[e]
        sine = sb_ref[...] * tc_ref[e] + cb_ref[...] * ts_ref[e]
        ch, cl = split_bf16(cosine)
        sh, sl = split_bf16(sine)
        for target, c, s in ((mh, ch, sh), (ml, cl, sl)):
            target[e, 0:local, 0:local] = c
            target[e, 0:local, local:] = s
            target[e, local:, 0:local] = -s
            target[e, local:, local:] = c
        return carry

    lax.fori_loop(0, n, make_matrix, 0)

    def second(o, h):
        dest = lax.rem(me + o, n)
        return pltpu.make_async_remote_copy(
            src_ref=send2.at[h, dest],
            dst_ref=out_ref.at[h, me],
            send_sem=s2_sem.at[o, h],
            recv_sem=r2_sem.at[o, h],
            device_id={"tm": dest},
            device_id_type=MESH,
        )

    def own_second(h):
        return pltpu.make_async_copy(send2.at[h, me], out_ref.at[h, me], own2_sem.at[h])

    for h in range(halves):
        own_first(h).wait()
        if h == 0:
            for i in range(BLOCKS):
                each(lambda o: first(o, 0, i).wait_recv())
        else:
            each(lambda o: first(o, h, 0).wait_recv())

        def across(g, carry):
            at = pl.ds(pl.multiple_of(g * 8, 8), 8)
            zs = [(recv1[h, d, 0, at, :], recv1[h, d, 1, at, :]) for d in range(n)]
            for e, (re, im) in enumerate(small_fft(zs)):
                spec[e, 0, at, :] = re
                spec[e, 1, at, :] = im
            return carry

        lax.fori_loop(0, local // 8, across, 0)

        def within(e, carry):
            high, low = split_bf16(spec[e].reshape(2 * local, LANES))
            dot = functools.partial(jnp.dot, preferred_element_type=jnp.float32)
            value = dot(mh[e], high) + (dot(mh[e], low) + dot(ml[e], high))
            value = value.reshape(2, n, keep, LANES)
            for p in range(2):
                send2[h, :, e, p] = value[p]
            return carry

        lax.fori_loop(0, n, within, 0)
        each(lambda o: second(o, h).start())
        own_second(h).start()

    for i in range(BLOCKS):
        each(lambda o: first(o, 0, i).wait_send())
    for h in range(1, halves):
        each(lambda o: first(o, h, 0).wait_send())
    for h in range(halves):
        own_second(h).wait()
        each(lambda o: second(o, h).wait())


def project_kernel(
    n, local, chans, uniq, kept, got_ref, filt_ref, mm_ref, modes_ref, lay, part
):
    step = pl.program_id(0)
    per_chan = n // chans
    lane_tiles = uniq // LANES
    halves = lane_tiles // per_chan
    keep = local // n
    width = n * 2 * chans

    @pl.when(step == 0)
    def _():
        def place(e, carry):
            for h in range(halves):
                for j in range(n):
                    lt = (j % per_chan) * halves + h
                    for p in range(2):
                        start = (e * 2 + p) * chans + j // per_chan
                        lay[lt, pl.ds(start, keep, stride=width), :] = got_ref[h, j, e, p]
            return carry

        lax.fori_loop(0, n, place, 0)

    def one(m, carry):
        at = pl.multiple_of(step * width + m * 2 * chans, 2 * chans)
        real = jnp.zeros((kept, chans, LANES), jnp.float32)
        imag = jnp.zeros((kept, chans, LANES), jnp.float32)
        for lt in range(lane_tiles):
            cols = slice(lt * LANES, (lt + 1) * LANES)
            x0 = lay[lt, pl.ds(at, chans), :]
            x1 = lay[lt, pl.ds(at + chans, chans), :]
            mm_ref[m, 0, :, cols] = x0
            mm_ref[m, 1, :, cols] = x1
            x0 = x0.astype(jnp.bfloat16).astype(jnp.float32)[None]
            x1 = x1.astype(jnp.bfloat16).astype(jnp.float32)[None]
            f0 = filt_ref[m, 0, :, :, cols].astype(jnp.float32)
            f1 = filt_ref[m, 1, :, :, cols].astype(jnp.float32)
            real += f0 * x0 - f1 * x1
            imag += f0 * x1 + f1 * x0
        part[m, 0] = jnp.sum(real, axis=1)
        part[m, 1] = jnp.sum(imag, axis=1)
        return carry

    lax.fori_loop(0, n, one, 0)
    sums = part[...].reshape(n * 2 * kept, LANES)
    total = lax.dot_general(
        jnp.ones((8, LANES), jnp.float32), sums, NT,
        precision=lax.Precision.HIGHEST, preferred_element_type=jnp.float32,
    )
    modes_ref[0] = total[0:1]


def fits(n, local, chans, raw, uniq, kept):
    return (
        n % chans == 0
        and uniq % ((n // chans) * LANES) == 0
        and local % (8 * n) == 0
        and local % (8 * BLOCKS) == 0
        and local % LANES == 0
        and chans == 8
        and raw % LANES == 0
        and kept % 8 == 0
        and local == 8 * n
    )


def fused_device(visibilities, redundancy, mode_counts, filters):
    n = lax.axis_size("tm")
    local, _, chans, raw = visibilities.shape
    uniq, kept = filters.shape[4], filters.shape[2]
    halves = uniq // (n // chans) // LANES
    keep = local // n
    rows = local * 2 * chans
    vmem = pl.BlockSpec(memory_space=pltpu.VMEM)
    hbm = pl.BlockSpec(memory_space=pl.ANY)
    f32, bf16 = jnp.float32, jnp.bfloat16
    dma = pltpu.SemaphoreType.DMA
    got = pl.pallas_call(
        functools.partial(exchange_kernel, n, local, chans, uniq),
        out_shape=jax.ShapeDtypeStruct((halves, n, n, 2, keep, LANES), f32),
        in_specs=[hbm] + [vmem] * 5,
        out_specs=hbm,
        scratch_shapes=[
            pltpu.VMEM((BLOCKS, rows // BLOCKS, raw), f32),
            pltpu.VMEM((uniq, raw), bf16),
            pltpu.VMEM((uniq // LANES, rows // BLOCKS, LANES), f32),
            pltpu.VMEM((uniq // LANES, chans, 2, local, LANES), f32),
            pltpu.VMEM((halves, n, 2, local, LANES), f32),
            pltpu.VMEM((n, 2, local, LANES), f32),
            pltpu.VMEM((n, 2 * local, 2 * local), bf16),
            pltpu.VMEM((n, 2 * local, 2 * local), bf16),
            pltpu.VMEM((halves, n, n, 2, keep, LANES), f32),
            dma((BLOCKS,)),
            dma((n, BLOCKS + halves - 1)),
            dma((n, BLOCKS + halves - 1)),
            dma((n, halves)),
            dma((n, halves)),
            dma((halves,)),
            dma((halves,)),
        ],
        compiler_params=pltpu.CompilerParams(
            collective_id=0, has_side_effects=True, vmem_limit_bytes=60 * 2**20
        ),
        name="exchange",
    )(visibilities.reshape(rows, raw), redundancy.reshape(1, raw), *tables(n, local))
    width = n * 2 * chans
    mmodes, flat = pl.pallas_call(
        functools.partial(project_kernel, n, local, chans, uniq, kept),
        grid=(keep,),
        out_shape=(
            jax.ShapeDtypeStruct((local, 2, chans, uniq), f32),
            jax.ShapeDtypeStruct((keep, 1, n * 2 * kept), f32),
        ),
        in_specs=[
            pl.BlockSpec(got.shape, lambda k: (0,) * 6),
            pl.BlockSpec((n, 2, kept, chans, uniq), lambda k: (k, 0, 0, 0, 0)),
        ],
        out_specs=(
            pl.BlockSpec((n, 2, chans, uniq), lambda k: (k, 0, 0, 0)),
            pl.BlockSpec((1, 1, n * 2 * kept), lambda k: (k, 0, 0)),
        ),
        scratch_shapes=[
            pltpu.VMEM((uniq // LANES, keep * width, LANES), f32),
            pltpu.VMEM((n, 2, kept, LANES), f32),
        ],
        compiler_params=pltpu.CompilerParams(vmem_limit_bytes=56 * 2**20),
        name="project",
    )(got, filters)
    coefs = flat.reshape(local, 2, kept)
    kept_mask = lax.broadcasted_iota(jnp.int32, (local, kept), 1) < mode_counts[:, None]
    return mmodes, jnp.where(kept_mask[:, None, :], coefs, 0.0)


def phase_table(numer, period):
    phases = 2.0 * jnp.pi / period * numer.astype(jnp.float32)
    return (jnp.cos(phases), jnp.sin(phases))


def apply_stacked(cosine, sine_table, stacked, width):
    cos_part = jnp.dot(
        cosine, stacked, precision=lax.Precision.HIGHEST, preferred_element_type=jnp.float32
    )
    sin_part = jnp.dot(
        sine_table, stacked, precision=lax.Precision.HIGHEST, preferred_element_type=jnp.float32
    )
    real_out = cos_part[:, :width] + sin_part[:, width:]
    imag_out = cos_part[:, width:] - sin_part[:, :width]
    return jnp.concatenate([real_out, imag_out], axis=1)


def factored_transform(stacked, width):
    length = stacked.shape[0]
    radix_size = 64
    inner_size = length // radix_size
    outer_row = lax.broadcasted_iota(jnp.int32, (radix_size, radix_size), 0)
    outer_col = lax.broadcasted_iota(jnp.int32, (radix_size, radix_size), 1)
    cosine, sine_table = phase_table(outer_row * outer_col % radix_size, radix_size)
    grouped = stacked.reshape(radix_size, inner_size, 2, width)
    grouped = jnp.transpose(grouped, (0, 2, 1, 3)).reshape(radix_size, 2 * inner_size * width)
    section = apply_stacked(cosine, sine_table, grouped, inner_size * width)
    section = section.reshape(radix_size, 2, inner_size, width)
    section_real = section[:, 0]
    section_imag = section[:, 1]
    twist_row = lax.broadcasted_iota(jnp.int32, (radix_size, inner_size, 1), 0)
    twist_col = lax.broadcasted_iota(jnp.int32, (radix_size, inner_size, 1), 1)
    twist_cos, twist_sin = phase_table(twist_row * twist_col, length)
    turned_real = section_real * twist_cos + section_imag * twist_sin
    turned_imag = section_imag * twist_cos - section_real * twist_sin
    turned = jnp.stack([turned_real, turned_imag], axis=0)
    turned = jnp.transpose(turned, (2, 0, 1, 3)).reshape(inner_size, 2 * radix_size * width)
    inner_row = lax.broadcasted_iota(jnp.int32, (inner_size, inner_size), 0)
    inner_col = lax.broadcasted_iota(jnp.int32, (inner_size, inner_size), 1)
    cosine2, sine_table2 = phase_table(inner_row * inner_col % inner_size, inner_size)
    final = apply_stacked(cosine2, sine_table2, turned, radix_size * width)
    final = final.reshape(inner_size, 2, radix_size, width)
    return jnp.transpose(final, (0, 2, 1, 3)).reshape(length, 2 * width)


def transform(columns):
    length, _, width = columns.shape
    stacked = columns.reshape(length, 2 * width)
    result = factored_transform(stacked, width)
    scale = 1.0 / jnp.sqrt(jnp.float32(length))
    return (result * scale).reshape(length, 2, width)


def on_device(visibilities, redundancy, mode_counts, filters):
    groups = lax.axis_size("tm")
    local_times, _, channels, raw_count = visibilities.shape
    uniques = filters.shape[4]
    kept = filters.shape[2]
    if fits(groups, local_times, channels, raw_count, uniques, kept):
        return fused_device(visibilities, redundancy, mode_counts, filters)
    unique_block = uniques // groups
    members = (
        redundancy[:, None] == lax.broadcasted_iota(jnp.int32, (raw_count, uniques), 1)
    ).astype(jnp.float32)
    weights = members / jnp.sum(members, axis=0, keepdims=True)
    flat_rows = visibilities.reshape(local_times, 2 * channels, raw_count)
    blocked_weights = weights.reshape(raw_count, groups, unique_block)
    packed = jnp.einsum(
        "tqr,rjc->tjqc",
        flat_rows,
        blocked_weights,
        precision=lax.Precision.HIGHEST,
        preferred_element_type=jnp.float32,
    )
    packed = packed.reshape(local_times, groups, 2 * channels * unique_block)
    arrived = lax.all_to_all(packed, "tm", split_axis=1, concat_axis=0, tiled=True)
    length = arrived.shape[0]
    spectra = transform(arrived.reshape(length, 2, channels * unique_block))
    spectra = spectra.reshape(length, 1, 2 * channels * unique_block)
    regrouped = lax.all_to_all(spectra, "tm", split_axis=0, concat_axis=1, tiled=True)
    regrouped = regrouped.reshape(local_times, groups, 2, channels, unique_block)
    mmodes = jnp.transpose(regrouped, (0, 2, 3, 1, 4)).reshape(local_times, 2, channels, uniques)
    local_modes = mmodes.shape[0]
    rounded = mmodes.astype(jnp.bfloat16).reshape(local_modes, 2, channels * uniques)
    flat_filters = filters.reshape(local_modes, 2, kept, channels * uniques)
    products = jnp.einsum(
        "mpkc,mqc->mpqk", flat_filters, rounded, preferred_element_type=jnp.float32
    )
    real_out = products[:, 0, 0] - products[:, 1, 1]
    imag_out = products[:, 0, 1] + products[:, 1, 0]
    kept_mask = lax.broadcasted_iota(jnp.int32, (local_modes, kept), 1) < mode_counts[:, None]
    modes = jnp.where(kept_mask[:, None, :], jnp.stack([real_out, imag_out], axis=1), 0.0)
    return (mmodes, modes)


def solution(mesh):
    return jax.shard_map(
        on_device,
        mesh=mesh,
        in_specs=(P("tm", None, "grp", None), P("grp"), P("tm"), P("tm", None, None, "grp", None)),
        out_specs=(P("tm", None, "grp", None), P("tm", None, "grp")),
        check_vma=False,
    )
```

```python
import functools

import numpy as np
import jax
import jax.numpy as jnp
from jax import lax
from jax.experimental import pallas as pl
from jax.experimental.pallas import tpu as pltpu
from jax.sharding import PartitionSpec as P

MESH = pl.DeviceIdType.MESH
LANES = 128
BLOCKS = 4
NT = (((1,), (1,)), ((), ()))


def split_bf16(x):
    high = x.astype(jnp.bfloat16)
    return high, (x - high.astype(jnp.float32)).astype(jnp.bfloat16)


def cmul_const(z, c):
    re, im = z
    if c == 1:
        return z
    if c == -1j:
        return im, -re
    cr, ci = float(c.real), float(c.imag)
    if abs(abs(cr) - abs(ci)) < 1e-12:
        return (re - im) * cr if ci * cr > 0 else (re + im) * cr, (re + im) * cr if ci * cr > 0 else (im - re) * cr
    return re * cr - im * ci, re * ci + im * cr


def small_fft(zs):
    n = len(zs)
    if n == 1:
        return zs
    half = n // 2
    tops = [(a[0] + b[0], a[1] + b[1]) for a, b in zip(zs[:half], zs[half:])]
    lows = [(a[0] - b[0], a[1] - b[1]) for a, b in zip(zs[:half], zs[half:])]
    turned = []
    for i, z in enumerate(lows):
        if i == 0:
            c = 1
        elif 4 * i == n:
            c = -1j
        else:
            c = np.exp(-2j * np.pi * i / n)
        turned.append(cmul_const(z, c))
    even, odd = small_fft(tops), small_fft(turned)
    out = [None] * n
    out[0::2], out[1::2] = even, odd
    return out


def rounded(x):
    return x.astype(jnp.bfloat16).astype(jnp.float32)[None]


def late_tiles(n, chans, uniq):
    halves = uniq // (n // chans) // LANES
    return [t for t in range(uniq // LANES) if t % halves]


def tables(groups, local):
    length = groups * local
    s = np.arange(local, dtype=np.int64)
    base = 2 * np.pi * (np.outer(s, s) % local) / local
    turn = 2 * np.pi * np.outer(np.arange(groups, dtype=np.int64), s) / length
    scale = length ** -0.5
    f32 = lambda a: jnp.asarray(a.astype(np.float32))
    return (
        f32(np.cos(base) * scale),
        f32(np.sin(base) * scale),
        f32(np.cos(turn).reshape(groups, 1, local)),
        f32(np.sin(turn).reshape(groups, 1, local)),
    )


def exchange_kernel(
    n, local, chans, uniq, kept,
    vis_ref, filt_ref, red_ref, cb_ref, sb_ref, tc_ref, ts_ref, out_ref, part_ref,
    vis_buf, wt, avg, send1, recv1, spec, mh, ml, send2, filt, got, lay, part,
    load_sem, s1_sem, r1_sem, s2_sem, r2_sem, own1_sem, own2_sem, filt_sem, got_sem, part_sem,
):
    me = lax.axis_index("tm")
    halves = uniq // (n // chans) // LANES
    per_chan = n // chans
    tb = local // BLOCKS
    rows = tb * 2 * chans
    keep = local // n

    def load(i):
        return pltpu.make_async_copy(
            vis_ref.at[pl.ds(i * rows, rows), :], vis_buf.at[i], load_sem.at[i]
        )

    for i in range(BLOCKS):
        load(i).start()

    barrier = pltpu.get_barrier_semaphore()

    def greet(o, carry):
        pl.semaphore_signal(
            barrier, inc=1, device_id={"tm": lax.rem(me + o, n)}, device_id_type=MESH
        )
        return carry

    lax.fori_loop(1, n, greet, 0)

    wt[...] = (
        lax.broadcasted_iota(jnp.int32, wt.shape, 0) == red_ref[...]
    ).astype(jnp.float32).astype(jnp.bfloat16)
    ones = jnp.ones((8, wt.shape[1]), jnp.bfloat16)
    counts = lax.dot_general(ones, wt[...], NT, preferred_element_type=jnp.float32)
    inverse = 1.0 / counts[0:1]

    def slot(dest, h):
        return lax.rem(dest, per_chan) * halves + h, lax.div(dest, per_chan)

    def first(o, h, i):
        dest = lax.rem(me + o, n)
        lane_tile, chan = slot(dest, h)
        if h == 0:
            span = pl.ds(i * tb, tb)
            q = i
        else:
            span = pl.ds(0, local)
            q = BLOCKS + h - 1
        return pltpu.make_async_remote_copy(
            src_ref=send1.at[lane_tile, chan, :, span, :],
            dst_ref=recv1.at[h, me, :, span, :],
            send_sem=s1_sem.at[o, q],
            recv_sem=r1_sem.at[o, q],
            device_id={"tm": dest},
            device_id_type=MESH,
        )

    def own_first(h):
        lane_tile, chan = slot(me, h)
        return pltpu.make_async_copy(
            send1.at[lane_tile, chan], recv1.at[h, me], own1_sem.at[h]
        )

    def each(f):
        def body(o, carry):
            f(o)
            return carry
        lax.fori_loop(1, n, body, 0)

    for i in range(BLOCKS):
        load(i).wait()
        high, low = split_bf16(vis_buf[i])
        summed = lax.dot_general(high, wt[...], NT, preferred_element_type=jnp.float32)
        summed += lax.dot_general(low, wt[...], NT, preferred_element_type=jnp.float32)
        mean = summed * inverse
        for lt in range(uniq // LANES):
            avg[lt] = mean[:, lt * LANES:(lt + 1) * LANES]
        for lt in range(uniq // LANES):
            for f in range(chans):
                for p in range(2):
                    send1[lt, f, p, i * tb:(i + 1) * tb, :] = avg[
                        lt, pl.ds(p * chans + f, tb, stride=2 * chans), :
                    ]
        if i == 0:
            pl.semaphore_wait(barrier, n - 1)
        each(lambda o: first(o, 0, i).start())
    for h in range(1, halves):
        each(lambda o: first(o, h, 0).start())
    for h in range(halves):
        own_first(h).start()

    def fetch(k, c):
        return pltpu.make_async_copy(
            filt_ref.at[pl.ds(k * n, n), :, :, :, pl.ds(c * halves * LANES, LANES)],
            filt.at[k, c],
            filt_sem.at[k, c],
        )

    for k in range(keep):
        for c in range(per_chan):
            fetch(k, c).start()

    def make_matrix(e, carry):
        cosine = cb_ref[...] * tc_ref[e] - sb_ref[...] * ts_ref[e]
        sine = sb_ref[...] * tc_ref[e] + cb_ref[...] * ts_ref[e]
        ch, cl = split_bf16(cosine)
        sh, sl = split_bf16(sine)
        for target, c, s in ((mh, ch, sh), (ml, cl, sl)):
            target[e, 0:local, 0:local] = c
            target[e, 0:local, local:] = s
            target[e, local:, 0:local] = -s
            target[e, local:, local:] = c
        return carry

    lax.fori_loop(0, n, make_matrix, 0)

    def second(o, h):
        dest = lax.rem(me + o, n)
        return pltpu.make_async_remote_copy(
            src_ref=send2.at[h, dest],
            dst_ref=out_ref.at[h, me],
            send_sem=s2_sem.at[o, h],
            recv_sem=r2_sem.at[o, h],
            device_id={"tm": dest},
            device_id_type=MESH,
        )

    def own_second(h):
        return pltpu.make_async_copy(send2.at[h, me], out_ref.at[h, me], own2_sem.at[h])

    for h in range(halves):
        own_first(h).wait()
        if h == 0:
            for i in range(BLOCKS):
                each(lambda o: first(o, 0, i).wait_recv())
        else:
            each(lambda o: first(o, h, 0).wait_recv())

        def across(g, carry):
            at = pl.ds(pl.multiple_of(g * 8, 8), 8)
            zs = [(recv1[h, d, 0, at, :], recv1[h, d, 1, at, :]) for d in range(n)]
            for e, (re, im) in enumerate(small_fft(zs)):
                spec[e, 0, at, :] = re
                spec[e, 1, at, :] = im
            return carry

        lax.fori_loop(0, local // 8, across, 0)

        def within(e, carry):
            high, low = split_bf16(spec[e].reshape(2 * local, LANES))
            dot = functools.partial(jnp.dot, preferred_element_type=jnp.float32)
            value = dot(mh[e], high) + (dot(mh[e], low) + dot(ml[e], high))
            value = value.reshape(2, n, keep, LANES)
            for p in range(2):
                send2[h, :, e, p] = value[p]
            return carry

        lax.fori_loop(0, n, within, 0)
        each(lambda o: second(o, h).start())
        own_second(h).start()

    own_second(0).wait()
    each(lambda o: second(o, 0).wait_recv())
    read = pltpu.make_async_copy(out_ref.at[0], got, got_sem)
    read.start()
    read.wait()
    width = n * 2 * chans

    def place(e, carry):
        for j in range(n):
            for p in range(2):
                start = (e * 2 + p) * chans + j // per_chan
                lay[j % per_chan, pl.ds(start, keep, stride=width), :] = got[j, e, p]
        return carry

    lax.fori_loop(0, n, place, 0)

    def early(k, carry):
        for c in range(per_chan):
            fetch(k, c).wait()

        def one(m, inner):
            at = pl.multiple_of(k * width + m * 2 * chans, 2 * chans)
            real = jnp.zeros((kept, chans, LANES), jnp.float32)
            imag = jnp.zeros((kept, chans, LANES), jnp.float32)
            for c in range(per_chan):
                x0 = rounded(lay[c, pl.ds(at, chans), :])
                x1 = rounded(lay[c, pl.ds(at + chans, chans), :])
                f0 = filt[k, c, m, 0].astype(jnp.float32)
                f1 = filt[k, c, m, 1].astype(jnp.float32)
                real += f0 * x0 - f1 * x1
                imag += f0 * x1 + f1 * x0
            part[k * n + m, 0] = jnp.sum(real, axis=1)
            part[k * n + m, 1] = jnp.sum(imag, axis=1)
            return inner

        lax.fori_loop(0, n, one, 0)
        return carry

    lax.fori_loop(0, keep, early, 0)
    save = pltpu.make_async_copy(part, part_ref, part_sem)
    save.start()

    for i in range(BLOCKS):
        each(lambda o: first(o, 0, i).wait_send())
    for h in range(1, halves):
        each(lambda o: first(o, h, 0).wait_send())
    each(lambda o: second(o, 0).wait_send())
    for h in range(1, halves):
        own_second(h).wait()
        each(lambda o: second(o, h).wait())
    save.wait()


def project_kernel(
    n, local, chans, uniq, kept, got_ref, early_ref, *refs
):
    late = late_tiles(n, chans, uniq)
    filt_refs = dict(zip(late, refs))
    mm_ref, modes_ref, lay, part = refs[len(late):]
    step = pl.program_id(0)
    per_chan = n // chans
    lane_tiles = uniq // LANES
    halves = lane_tiles // per_chan
    keep = local // n
    width = n * 2 * chans

    @pl.when(step == 0)
    def _():
        def place(e, carry):
            for h in range(halves):
                for j in range(n):
                    lt = (j % per_chan) * halves + h
                    for p in range(2):
                        start = (e * 2 + p) * chans + j // per_chan
                        lay[lt, pl.ds(start, keep, stride=width), :] = got_ref[h, j, e, p]
            return carry

        lax.fori_loop(0, n, place, 0)

    def one(m, carry):
        at = pl.multiple_of(step * width + m * 2 * chans, 2 * chans)
        real = jnp.zeros((kept, chans, LANES), jnp.float32)
        imag = jnp.zeros((kept, chans, LANES), jnp.float32)
        for lt in range(lane_tiles):
            cols = slice(lt * LANES, (lt + 1) * LANES)
            x0 = lay[lt, pl.ds(at, chans), :]
            x1 = lay[lt, pl.ds(at + chans, chans), :]
            mm_ref[m, 0, :, cols] = x0
            mm_ref[m, 1, :, cols] = x1
            if lt not in filt_refs:
                continue
            x0, x1 = rounded(x0), rounded(x1)
            f0 = filt_refs[lt][m, 0].astype(jnp.float32)
            f1 = filt_refs[lt][m, 1].astype(jnp.float32)
            real += f0 * x0 - f1 * x1
            imag += f0 * x1 + f1 * x0
        part[m, 0] = jnp.sum(real, axis=1) + early_ref[m, 0]
        part[m, 1] = jnp.sum(imag, axis=1) + early_ref[m, 1]
        return carry

    lax.fori_loop(0, n, one, 0)
    sums = part[...].reshape(n * 2 * kept, LANES)
    total = lax.dot_general(
        jnp.ones((8, LANES), jnp.float32), sums, NT,
        precision=lax.Precision.HIGHEST, preferred_element_type=jnp.float32,
    )
    modes_ref[0] = total[0:1]


def fits(n, local, chans, raw, uniq, kept):
    return (
        n % chans == 0
        and uniq % ((n // chans) * LANES) == 0
        and local % (8 * n) == 0
        and local % (8 * BLOCKS) == 0
        and local % LANES == 0
        and chans == 8
        and raw % LANES == 0
        and kept % 8 == 0
        and local == 8 * n
    )


def fused_device(visibilities, redundancy, mode_counts, filters):
    n = lax.axis_size("tm")
    local, _, chans, raw = visibilities.shape
    uniq, kept = filters.shape[4], filters.shape[2]
    halves = uniq // (n // chans) // LANES
    keep = local // n
    rows = local * 2 * chans
    vmem = pl.BlockSpec(memory_space=pltpu.VMEM)
    hbm = pl.BlockSpec(memory_space=pl.ANY)
    f32, bf16 = jnp.float32, jnp.bfloat16
    dma = pltpu.SemaphoreType.DMA
    per_chan = n // chans
    late = late_tiles(n, chans, uniq)
    got, early = pl.pallas_call(
        functools.partial(exchange_kernel, n, local, chans, uniq, kept),
        out_shape=(
            jax.ShapeDtypeStruct((halves, n, n, 2, keep, LANES), f32),
            jax.ShapeDtypeStruct((local, 2, kept, LANES), f32),
        ),
        in_specs=[hbm] * 2 + [vmem] * 5,
        out_specs=(hbm, hbm),
        scratch_shapes=[
            pltpu.VMEM((BLOCKS, rows // BLOCKS, raw), f32),
            pltpu.VMEM((uniq, raw), bf16),
            pltpu.VMEM((uniq // LANES, rows // BLOCKS, LANES), f32),
            pltpu.VMEM((uniq // LANES, chans, 2, local, LANES), f32),
            pltpu.VMEM((halves, n, 2, local, LANES), f32),
            pltpu.VMEM((n, 2, local, LANES), f32),
            pltpu.VMEM((n, 2 * local, 2 * local), bf16),
            pltpu.VMEM((n, 2 * local, 2 * local), bf16),
            pltpu.VMEM((halves, n, n, 2, keep, LANES), f32),
            pltpu.VMEM((keep, per_chan, n, 2, kept, chans, LANES), bf16),
            pltpu.VMEM((n, n, 2, keep, LANES), f32),
            pltpu.VMEM((per_chan, rows, LANES), f32),
            pltpu.VMEM((local, 2, kept, LANES), f32),
            dma((BLOCKS,)),
            dma((n, BLOCKS + halves - 1)),
            dma((n, BLOCKS + halves - 1)),
            dma((n, halves)),
            dma((n, halves)),
            dma((halves,)),
            dma((halves,)),
            dma((keep, per_chan)),
            dma,
            dma,
        ],
        compiler_params=pltpu.CompilerParams(
            collective_id=0, has_side_effects=True, vmem_limit_bytes=60 * 2**20
        ),
        name="exchange",
    )(visibilities.reshape(rows, raw), filters, redundancy.reshape(1, raw), *tables(n, local))
    width = n * 2 * chans
    mmodes, flat = pl.pallas_call(
        functools.partial(project_kernel, n, local, chans, uniq, kept),
        grid=(keep,),
        out_shape=(
            jax.ShapeDtypeStruct((local, 2, chans, uniq), f32),
            jax.ShapeDtypeStruct((keep, 1, n * 2 * kept), f32),
        ),
        in_specs=[
            pl.BlockSpec(got.shape, lambda k: (0,) * 6),
            pl.BlockSpec((n, 2, kept, LANES), lambda k: (k, 0, 0, 0)),
        ]
        + [
            pl.BlockSpec((n, 2, kept, chans, LANES), functools.partial(lambda t, k: (k, 0, 0, 0, t), t))
            for t in late
        ],
        out_specs=(
            pl.BlockSpec((n, 2, chans, uniq), lambda k: (k, 0, 0, 0)),
            pl.BlockSpec((1, 1, n * 2 * kept), lambda k: (k, 0, 0)),
        ),
        scratch_shapes=[
            pltpu.VMEM((uniq // LANES, keep * width, LANES), f32),
            pltpu.VMEM((n, 2, kept, LANES), f32),
        ],
        compiler_params=pltpu.CompilerParams(vmem_limit_bytes=56 * 2**20),
        name="project",
    )(got, early, *[filters] * len(late))
    coefs = flat.reshape(local, 2, kept)
    kept_mask = lax.broadcasted_iota(jnp.int32, (local, kept), 1) < mode_counts[:, None]
    return mmodes, jnp.where(kept_mask[:, None, :], coefs, 0.0)


def phase_table(numer, period):
    phases = 2.0 * jnp.pi / period * numer.astype(jnp.float32)
    return (jnp.cos(phases), jnp.sin(phases))


def apply_stacked(cosine, sine_table, stacked, width):
    cos_part = jnp.dot(
        cosine, stacked, precision=lax.Precision.HIGHEST, preferred_element_type=jnp.float32
    )
    sin_part = jnp.dot(
        sine_table, stacked, precision=lax.Precision.HIGHEST, preferred_element_type=jnp.float32
    )
    real_out = cos_part[:, :width] + sin_part[:, width:]
    imag_out = cos_part[:, width:] - sin_part[:, :width]
    return jnp.concatenate([real_out, imag_out], axis=1)


def factored_transform(stacked, width):
    length = stacked.shape[0]
    radix_size = 64
    inner_size = length // radix_size
    outer_row = lax.broadcasted_iota(jnp.int32, (radix_size, radix_size), 0)
    outer_col = lax.broadcasted_iota(jnp.int32, (radix_size, radix_size), 1)
    cosine, sine_table = phase_table(outer_row * outer_col % radix_size, radix_size)
    grouped = stacked.reshape(radix_size, inner_size, 2, width)
    grouped = jnp.transpose(grouped, (0, 2, 1, 3)).reshape(radix_size, 2 * inner_size * width)
    section = apply_stacked(cosine, sine_table, grouped, inner_size * width)
    section = section.reshape(radix_size, 2, inner_size, width)
    section_real = section[:, 0]
    section_imag = section[:, 1]
    twist_row = lax.broadcasted_iota(jnp.int32, (radix_size, inner_size, 1), 0)
    twist_col = lax.broadcasted_iota(jnp.int32, (radix_size, inner_size, 1), 1)
    twist_cos, twist_sin = phase_table(twist_row * twist_col, length)
    turned_real = section_real * twist_cos + section_imag * twist_sin
    turned_imag = section_imag * twist_cos - section_real * twist_sin
    turned = jnp.stack([turned_real, turned_imag], axis=0)
    turned = jnp.transpose(turned, (2, 0, 1, 3)).reshape(inner_size, 2 * radix_size * width)
    inner_row = lax.broadcasted_iota(jnp.int32, (inner_size, inner_size), 0)
    inner_col = lax.broadcasted_iota(jnp.int32, (inner_size, inner_size), 1)
    cosine2, sine_table2 = phase_table(inner_row * inner_col % inner_size, inner_size)
    final = apply_stacked(cosine2, sine_table2, turned, radix_size * width)
    final = final.reshape(inner_size, 2, radix_size, width)
    return jnp.transpose(final, (0, 2, 1, 3)).reshape(length, 2 * width)


def transform(columns):
    length, _, width = columns.shape
    stacked = columns.reshape(length, 2 * width)
    result = factored_transform(stacked, width)
    scale = 1.0 / jnp.sqrt(jnp.float32(length))
    return (result * scale).reshape(length, 2, width)


def on_device(visibilities, redundancy, mode_counts, filters):
    groups = lax.axis_size("tm")
    local_times, _, channels, raw_count = visibilities.shape
    uniques = filters.shape[4]
    kept = filters.shape[2]
    if fits(groups, local_times, channels, raw_count, uniques, kept):
        return fused_device(visibilities, redundancy, mode_counts, filters)
    unique_block = uniques // groups
    members = (
        redundancy[:, None] == lax.broadcasted_iota(jnp.int32, (raw_count, uniques), 1)
    ).astype(jnp.float32)
    weights = members / jnp.sum(members, axis=0, keepdims=True)
    flat_rows = visibilities.reshape(local_times, 2 * channels, raw_count)
    blocked_weights = weights.reshape(raw_count, groups, unique_block)
    packed = jnp.einsum(
        "tqr,rjc->tjqc",
        flat_rows,
        blocked_weights,
        precision=lax.Precision.HIGHEST,
        preferred_element_type=jnp.float32,
    )
    packed = packed.reshape(local_times, groups, 2 * channels * unique_block)
    arrived = lax.all_to_all(packed, "tm", split_axis=1, concat_axis=0, tiled=True)
    length = arrived.shape[0]
    spectra = transform(arrived.reshape(length, 2, channels * unique_block))
    spectra = spectra.reshape(length, 1, 2 * channels * unique_block)
    regrouped = lax.all_to_all(spectra, "tm", split_axis=0, concat_axis=1, tiled=True)
    regrouped = regrouped.reshape(local_times, groups, 2, channels, unique_block)
    mmodes = jnp.transpose(regrouped, (0, 2, 3, 1, 4)).reshape(local_times, 2, channels, uniques)
    local_modes = mmodes.shape[0]
    rounded = mmodes.astype(jnp.bfloat16).reshape(local_modes, 2, channels * uniques)
    flat_filters = filters.reshape(local_modes, 2, kept, channels * uniques)
    products = jnp.einsum(
        "mpkc,mqc->mpqk", flat_filters, rounded, preferred_element_type=jnp.float32
    )
    real_out = products[:, 0, 0] - products[:, 1, 1]
    imag_out = products[:, 0, 1] + products[:, 1, 0]
    kept_mask = lax.broadcasted_iota(jnp.int32, (local_modes, kept), 1) < mode_counts[:, None]
    modes = jnp.where(kept_mask[:, None, :], jnp.stack([real_out, imag_out], axis=1), 0.0)
    return (mmodes, modes)


def solution(mesh):
    return jax.shard_map(
        on_device,
        mesh=mesh,
        in_specs=(P("tm", None, "grp", None), P("grp"), P("tm"), P("tm", None, None, "grp", None)),
        out_specs=(P("tm", None, "grp", None), P("tm", None, "grp")),
        check_vma=False,
    )
```
